32 devices in a mesh: dp: 8 (over y, x, core), group: 4 (over z).
Axes of the slice: x: 2, y: 2, z: 4, core: 2. Of those that a mesh axis runs over, the one named last changes fastest.
Arguments:
- images: bfloat16 [4096, 512], P(('dp', 'group')), may hold values from -1 to 1
- texts: bfloat16 [4096, 512], P(('dp', 'group')), may hold values from -1 to 1
- log_scale: float32 [], replicated, may hold values from 2 to 2.7
Outputs:
- grad_images: bfloat16 [4096, 512], P(('dp', 'group'))
- grad_texts: bfloat16 [4096, 512], P(('dp', 'group'))
- loss: float32 [], replicated
- grad_scale: float32 [], replicated
The draws below stay inside these ranges and needn't reach their ends.
All inputs are finite; a program needn't handle non-finite values.
Results may differ from the reference program's by a relative error of at most 0.0013.
The reference program's roundings to bfloat16 on the way (of `weights_low`) count: a program that leaves them out, or rounds other values in their place, can miss the bound.
Values may be sent and summed in bfloat16 or wider, within the bound.
A program may use at most 128 MiB of HBM per device.

```python
import jax
import jax.numpy as jnp
from jax import lax

D = 512
B_DEV = 128
N = 4096


def draw_pair(key):
    spread_dims = jnp.exp(jax.random.uniform(jax.random.fold_in(key, 17), (1, D), jnp.float32, -0.693, 0.693))
    spread_dims = spread_dims / jnp.sqrt(jnp.mean(spread_dims * spread_dims))
    base = jnp.clip(0.05 * spread_dims * jax.random.normal(jax.random.fold_in(key, 11), (N, D), jnp.float32), -0.5, 0.5)
    noise = jnp.clip(0.05 * spread_dims * jax.random.normal(jax.random.fold_in(key, 12), (N, D), jnp.float32), -0.5, 0.5)
    paired = 0.3 * base + 0.95 * noise
    common = 0.05 * jax.random.rademacher(jax.random.fold_in(key, 16), (1, D), jnp.float32)
    image_share = jax.random.uniform(jax.random.fold_in(key, 18), (N, 1), jnp.float32, 0.1, 0.4)
    text_share = jax.random.uniform(jax.random.fold_in(key, 19), (N, 1), jnp.float32, 0.1, 0.4)
    base = base + image_share * common
    paired = paired + text_share * common
    return (jnp.clip(base, -1.0, 1.0), jnp.clip(paired, -1.0, 1.0))


def draw_images(key, part):
    return draw_pair(key)[0].astype(jnp.bfloat16)


def draw_texts(key, part):
    return draw_pair(key)[1].astype(jnp.bfloat16)


def setup_inputs(seed: int = 0) -> dict:
    streams_of = jax.random.split(jax.random.key(seed), 4)
    images = draw_images(jax.random.fold_in(streams_of[3], 71), 0)
    texts = draw_texts(jax.random.fold_in(streams_of[3], 71), 0)
    log_scale = jnp.clip(jax.random.uniform(streams_of[2], (), jnp.float32, 2.0, 2.7), 2.0, 2.7)
    return dict(images=images, texts=texts, log_scale=log_scale)


def reference(images, texts, log_scale):
    pair_total = images.shape[0]
    block_rows = B_DEV
    block_count = pair_total // block_rows
    logit_scale = jnp.exp(log_scale)
    columns = jnp.arange(pair_total).astype(jnp.int32)

    def logits_at(block_index):
        first_row = (block_index * block_rows).astype(jnp.int32)
        image_rows = lax.dynamic_slice_in_dim(images, first_row, block_rows, 0)
        logits = logit_scale * jnp.dot(image_rows, texts.T, preferred_element_type=jnp.float32)
        return image_rows, first_row, logits

    def first_pass(carry, block_index):
        col_top, col_sum = carry
        image_rows, first_row, logits = logits_at(block_index)
        row_top = jnp.max(logits, axis=1)
        row_lse = row_top + jnp.log(jnp.sum(jnp.exp(logits - row_top[:, None]), axis=1))
        paired = jnp.diagonal(lax.dynamic_slice_in_dim(logits, first_row, block_rows, 1))
        new_top = jnp.maximum(col_top, jnp.max(logits, axis=0))
        col_sum = col_sum * jnp.exp(col_top - new_top) + jnp.sum(jnp.exp(logits - new_top[None, :]), axis=0)
        return (new_top, col_sum), (row_lse, paired)

    start_carry = (jnp.full((pair_total,), -1e30, jnp.float32), jnp.zeros((pair_total,), jnp.float32))
    indices = jnp.arange(block_count).astype(jnp.int32)
    (col_top, col_sum), (row_lse, paired) = lax.scan(first_pass, start_carry, indices)
    col_lse = col_top + jnp.log(col_sum)

    def second_pass(carry, inputs):
        text_sum, scale_sum = carry
        block_index, block_lse = inputs
        image_rows, first_row, logits = logits_at(block_index)
        own_pairs = (columns[None, :] == (first_row + jnp.arange(block_rows).astype(jnp.int32))[:, None]).astype(jnp.float32)
        grad_block = 0.5 * (jnp.exp(logits - block_lse[:, None]) + jnp.exp(logits - col_lse[None, :])) - own_pairs
        scale_sum = scale_sum + jnp.sum(grad_block * logits)
        weights_low = grad_block.astype(jnp.bfloat16)
        image_grad = logit_scale * jnp.dot(weights_low, texts, preferred_element_type=jnp.float32)
        text_sum = text_sum + jnp.dot(weights_low.T, image_rows, preferred_element_type=jnp.float32)
        return (text_sum, scale_sum), image_grad.astype(jnp.bfloat16)

    start_two = (jnp.zeros(texts.shape, jnp.float32), jnp.zeros((), jnp.float32))
    (text_sum, scale_sum), image_blocks = lax.scan(second_pass, start_two, (indices, row_lse))
    grad_images = image_blocks.reshape(pair_total, images.shape[1])
    grad_texts = (logit_scale * text_sum).astype(jnp.bfloat16)
    loss = (jnp.sum(row_lse) + jnp.sum(col_lse) - 2.0 * jnp.sum(paired)) / (2.0 * pair_total)
    grad_scale = scale_sum / pair_total
    return grad_images, grad_texts, loss, grad_scale
```

```python
import functools

import jax
import jax.numpy as jnp
from jax import lax
from jax.experimental import pallas as pl
from jax.experimental.pallas import tpu as pltpu
from jax.sharding import PartitionSpec as P

MESH = pl.DeviceIdType.MESH
NT = (((1,), (1,)), ((), ()))
NN = (((1,), (0,)), ((), ()))
TN = (((0,), (0,)), ((), ()))
F32 = jnp.float32
BLOCK, STAT, GRAD, SCALAR = range(4)


def each(count, step):
    if count <= 8:
        for i in range(count):
            step(i)
    else:
        lax.fori_loop(0, count, lambda i, c: (step(i), c)[1], 0)


def kernel(
    gn, dn, images, texts, log_scale, gi_out, gt_out, loss_out, scale_out,
    img_all, txt_all, logits, weights, row_stat, col_stat, top, acc, row_lse, col_lse,
    gi_send, gi_recv, gt_send, gt_recv, sc_group, sc_dp, g_send, g_recv, d_send, d_recv,
):
    rows, width = images.shape
    g = lax.axis_index("group")
    d = lax.axis_index("dp")
    wide = 2 * rows if dn % 2 == 0 else rows
    per = wide // rows
    chunks = dn // per

    def g_peer(o):
        return lax.rem(g + o, gn)

    def d_peer(o):
        return lax.rem(d + o, dn)

    def at(k, n=rows):
        return pl.ds(pl.multiple_of(k * n, n), n)

    def g_copy(kind, src, dst, to, slot):
        return pltpu.make_async_remote_copy(
            src_ref=src, dst_ref=dst, send_sem=g_send.at[kind, to], recv_sem=g_recv.at[kind, slot],
            device_id={"group": to}, device_id_type=MESH)

    def d_copy(kind, src, dst, to, slot):
        return pltpu.make_async_remote_copy(
            src_ref=src, dst_ref=dst, send_sem=d_send.at[kind, to], recv_sem=d_recv.at[kind, slot],
            device_id={"dp": to}, device_id_type=MESH)

    barrier = pltpu.get_barrier_semaphore()
    each(gn - 1, lambda i: pl.semaphore_signal(
        barrier, inc=1, device_id={"group": g_peer(i + 1)}, device_id_type=MESH))
    each(dn - 1, lambda i: pl.semaphore_signal(
        barrier, inc=1, device_id={"dp": d_peer(i + 1)}, device_id_type=MESH))
    pl.semaphore_wait(barrier, gn + dn - 2)

    each(gn - 1, lambda i: g_copy(BLOCK, images, img_all.at[at(g)], g_peer(i + 1), g).start())
    each(dn - 1, lambda i: d_copy(BLOCK, texts, txt_all.at[at(d)], d_peer(i + 1), d).start())
    img_all[at(g), :] = images[...]
    txt_all[at(d), :] = texts[...]
    s = jnp.exp(log_scale[...])
    eye = (lax.broadcasted_iota(jnp.int32, (rows, rows), 0)
           == lax.broadcasted_iota(jnp.int32, (rows, rows), 1))

    def wait_image(i):
        k = g_peer(i + 1)
        g_copy(BLOCK, images, img_all.at[at(k)], k, k).wait_recv()

    each(gn - 1, wait_image)

    def logits_chunk(i):
        c = lax.rem(d // per + i, chunks)

        def wait_text(j):
            k = c * per + j

            @pl.when(k != d)
            def _():
                d_copy(BLOCK, texts, txt_all.at[at(k)], k, k).wait_recv()

        each(per, wait_text)
        part = s * lax.dot_general(img_all[...], txt_all[at(c, wide), :], NT, preferred_element_type=F32)
        logits[:, at(c, wide)] = part
        high = jnp.max(part, axis=0, keepdims=True)
        col_stat[d, 0:1, at(c, wide)] = high
        col_stat[d, 1:2, at(c, wide)] = jnp.sum(jnp.exp(part - high), axis=0, keepdims=True)
        if isinstance(i, int) and i == 0:
            top[...] = part
        else:
            top[...] = jnp.maximum(top[...], part)

    if chunks > 8:
        top[...] = jnp.full(top.shape, -jnp.inf, F32)
    each(chunks, logits_chunk)
    each(dn - 1, lambda i: d_copy(STAT, col_stat.at[d], col_stat.at[d], d_peer(i + 1), d).start())

    def flat(col):
        return jnp.sum(jnp.where(eye, col, 0.0), axis=0, keepdims=True)

    def stand(line):
        return jnp.sum(jnp.where(eye, line, 0.0), axis=1, keepdims=True)

    for k in range(gn):
        band = pl.ds(k * rows, rows)
        high = jnp.max(top[band, :], axis=1, keepdims=True)
        acc[...] = jnp.zeros(acc.shape, F32)

        def add(c):
            acc[...] += jnp.exp(logits[band, at(c, wide)] - high)

        each(chunks, add)
        row_stat[g, 0:1, band] = flat(high)
        row_stat[g, 1:2, band] = flat(jnp.sum(acc[...], axis=1, keepdims=True))
    each(gn - 1, lambda i: g_copy(STAT, row_stat.at[g], row_stat.at[g], g_peer(i + 1), g).start())

    def wait_row(i):
        k = g_peer(i + 1)
        g_copy(STAT, row_stat.at[k], row_stat.at[k], k, k).wait_recv()

    def wait_col(i):
        k = d_peer(i + 1)
        d_copy(STAT, col_stat.at[k], col_stat.at[k], k, k).wait_recv()

    def lse(stat):
        high = jnp.max(stat[:, 0, :], axis=0, keepdims=True)
        return high + jnp.log(jnp.sum(stat[:, 1, :] * jnp.exp(stat[:, 0, :] - high), axis=0, keepdims=True))

    each(dn - 1, wait_col)
    col_lse[...] = lse(col_stat)
    each(gn - 1, wait_row)
    row_lse[...] = lse(row_stat)

    acc[...] = jnp.zeros(acc.shape, F32)
    step_of = (lax.broadcasted_iota(jnp.int32, (rows, wide), 1)
               - lax.broadcasted_iota(jnp.int32, (rows, wide), 0))
    for o in [*range(1, gn), 0]:
        k = g_peer(o)
        line = stand(row_lse[0:1, at(k)])

        def weigh(c):
            part = logits[at(k), at(c, wide)]
            w = 0.5 * (jnp.exp(part - line) + jnp.exp(part - col_lse[0:1, at(c, wide)]))
            if o == 0:
                w = w - jnp.where(step_of == d * rows - c * wide, 1.0, 0.0)
            acc[...] += w * part
            weights[at(k), at(c, wide)] = w.astype(jnp.bfloat16)

        each(chunks, weigh)
        gi_send[k] = lax.dot_general(weights[at(k), :], txt_all[...], NN, preferred_element_type=F32)
        if o:
            g_copy(GRAD, gi_send.at[k], gi_recv.at[g], k, g).start()

    own = logits[at(g), at(d)]
    pairs = jnp.sum(jnp.where(eye, own, 0.0), axis=0, keepdims=True)
    loss_part = jnp.sum(row_lse[0:1, at(g)] + col_lse[0:1, at(d)] - 2.0 * pairs, axis=1, keepdims=True)
    scale_part = jnp.sum(jnp.sum(acc[...], axis=0, keepdims=True), axis=1, keepdims=True)
    first = lax.broadcasted_iota(jnp.int32, (8, 128), 1) == 0
    sc_group[g] = jnp.where(first, loss_part, scale_part)
    each(gn - 1, lambda i: g_copy(SCALAR, sc_group.at[g], sc_group.at[g], g_peer(i + 1), g).start())

    def text_chunk(i):
        c = lax.rem(d // per + 1 + i, chunks)
        part = lax.dot_general(weights[:, at(c, wide)], img_all[...], TN, preferred_element_type=F32)
        for j in range(per):
            k = c * per + j
            gt_send[k] = part[j * rows:(j + 1) * rows]

            @pl.when(k != d)
            def _():
                d_copy(GRAD, gt_send.at[k], gt_recv.at[d], k, d).start()

    each(chunks, text_chunk)

    def wait_sc_group(i):
        k = g_peer(i + 1)
        g_copy(SCALAR, sc_group.at[k], sc_group.at[k], k, k).wait_recv()

    each(gn - 1, wait_sc_group)
    sc_dp[d] = jnp.sum(sc_group[...], axis=0)
    each(dn - 1, lambda i: d_copy(SCALAR, sc_dp.at[d], sc_dp.at[d], d_peer(i + 1), d).start())

    def take_g(i):
        k = g_peer(i + 1)
        g_copy(GRAD, gi_send.at[k], gi_recv.at[k], k, k).wait_recv()
        gi_send[g] += gi_recv[k]

    def take_d(i):
        k = d_peer(i + 1)
        d_copy(GRAD, gt_send.at[k], gt_recv.at[k], k, k).wait_recv()
        gt_send[d] += gt_recv[k]

    each(gn - 1, take_g)
    gi_out[...] = (s * gi_send[g]).astype(gi_out.dtype)
    each(dn - 1, take_d)
    gt_out[...] = (s * gt_send[d]).astype(gt_out.dtype)

    def wait_sc_dp(i):
        k = d_peer(i + 1)
        d_copy(SCALAR, sc_dp.at[k], sc_dp.at[k], k, k).wait_recv()

    each(dn - 1, wait_sc_dp)
    total = jnp.sum(sc_dp[...], axis=0)
    pair_total = gn * dn * rows
    loss_out[...] = total[0:1, 0:1] / (2.0 * pair_total)
    scale_out[...] = total[0:1, 1:2] / pair_total

    def end_g(i):
        k = g_peer(i + 1)
        g_copy(BLOCK, images, img_all.at[at(g)], k, g).wait_send()
        g_copy(STAT, row_stat.at[g], row_stat.at[g], k, g).wait_send()
        g_copy(GRAD, gi_send.at[k], gi_recv.at[g], k, g).wait_send()
        g_copy(SCALAR, sc_group.at[g], sc_group.at[g], k, g).wait_send()

    def end_d(i):
        k = d_peer(i + 1)
        d_copy(BLOCK, texts, txt_all.at[at(d)], k, d).wait_send()
        d_copy(STAT, col_stat.at[d], col_stat.at[d], k, d).wait_send()
        d_copy(GRAD, gt_send.at[k], gt_recv.at[d], k, d).wait_send()
        d_copy(SCALAR, sc_dp.at[d], sc_dp.at[d], k, d).wait_send()

    each(gn - 1, end_g)
    each(dn - 1, end_d)


def body(gn, dn, images, texts, log_scale):
    rows, width = images.shape
    high, across = gn * rows, dn * rows
    wide = 2 * rows if dn % 2 == 0 else rows
    vmem = pl.BlockSpec(memory_space=pltpu.VMEM)
    gi, gt, loss, scale = pl.pallas_call(
        functools.partial(kernel, gn, dn),
        out_shape=(
            jax.ShapeDtypeStruct(images.shape, images.dtype),
            jax.ShapeDtypeStruct(texts.shape, texts.dtype),
            jax.ShapeDtypeStruct((1, 1), F32),
            jax.ShapeDtypeStruct((1, 1), F32),
        ),
        in_specs=[vmem] * 3,
        out_specs=(vmem,) * 4,
        scratch_shapes=[
            pltpu.VMEM((high, width), images.dtype),
            pltpu.VMEM((across, width), texts.dtype),
            pltpu.VMEM((high, across), F32),
            pltpu.VMEM((high, across), jnp.bfloat16),
            pltpu.VMEM((gn, 2, high), F32),
            pltpu.VMEM((dn, 2, across), F32),
            pltpu.VMEM((high, wide), F32),
            pltpu.VMEM((rows, wide), F32),
            pltpu.VMEM((1, high), F32),
            pltpu.VMEM((1, across), F32),
            pltpu.VMEM((gn, rows, width), F32),
            pltpu.VMEM((gn, rows, width), F32),
            pltpu.VMEM((dn, rows, width), F32),
            pltpu.VMEM((dn, rows, width), F32),
            pltpu.VMEM((gn, 8, 128), F32),
            pltpu.VMEM((dn, 8, 128), F32),
            pltpu.SemaphoreType.DMA((4, gn)),
            pltpu.SemaphoreType.DMA((4, gn)),
            pltpu.SemaphoreType.DMA((4, dn)),
            pltpu.SemaphoreType.DMA((4, dn)),
        ],
        compiler_params=pltpu.CompilerParams(
            collective_id=0, has_side_effects=True, vmem_limit_bytes=60 * 1024 * 1024),
    )(images, texts, log_scale.reshape(1, 1))
    return gi, gt, loss.reshape(()), scale.reshape(())


def solution(mesh):
    gn, dn = mesh.shape["group"], mesh.shape["dp"]
    spec = P(("dp", "group"), None)
    return jax.shard_map(
        functools.partial(body, gn, dn), mesh=mesh, in_specs=(spec, spec, P()),
        out_specs=(spec, spec, P(), P()), check_vma=False)
```

```python
import functools

import jax
import jax.numpy as jnp
from jax import lax
from jax.experimental import pallas as pl
from jax.experimental.pallas import tpu as pltpu
from jax.sharding import PartitionSpec as P

MESH = pl.DeviceIdType.MESH
NT = (((1,), (1,)), ((), ()))
NN = (((1,), (0,)), ((), ()))
TN = (((0,), (0,)), ((), ()))
F32 = jnp.float32
BLOCK, STAT, GRAD, SCALAR = range(4)
UP, DOWN = range(2)
PIECES = 2


def each(count, step):
    if count <= 8:
        for i in range(count):
            step(i)
    else:
        lax.fori_loop(0, count, lambda i, c: (step(i), c)[1], 0)


def kernel(
    gn, dn, images, texts, log_scale, gi_out, gt_out, loss_out, scale_out,
    img_all, txt_all, logits, weights, row_stat, col_stat, top, acc, row_lse, col_lse,
    gi_send, gi_recv, gt_send, gt_recv, gt_side, sc_group, sc_dp, g_send, g_recv, d_send, d_recv,
    hop_send, sum_send, sum_recv, side_send, pass_send, side_recv,
):
    rows, width = images.shape
    g = lax.axis_index("group")
    d = lax.axis_index("dp")
    wide = 2 * rows if dn % 2 == 0 else rows
    per = wide // rows
    chunks = dn // per

    chip, core = d // per, lax.rem(d, per)
    side = chip * per + (per - 1 - core)
    next_g = (lax.min(g + 1, gn - 1), lax.max(g - 1, 0))

    def c_peer(o):
        return lax.rem(chip + o, chunks)

    def hop(way, k):
        return pltpu.make_async_remote_copy(
            src_ref=img_all.at[at(k)], dst_ref=img_all.at[at(k)],
            send_sem=hop_send.at[way, k], recv_sem=g_recv.at[BLOCK, k],
            device_id={"group": next_g[way]}, device_id_type=MESH)

    def first_hop(way):
        return pltpu.make_async_remote_copy(
            src_ref=images, dst_ref=img_all.at[at(g)],
            send_sem=hop_send.at[way, g], recv_sem=g_recv.at[BLOCK, g],
            device_id={"group": next_g[way]}, device_id_type=MESH)

    def sum_hop(way, k, p):
        piece = pl.ds(p * (rows // PIECES), rows // PIECES)
        return pltpu.make_async_remote_copy(
            src_ref=gi_send.at[k, piece], dst_ref=gi_recv.at[way, k, piece],
            send_sem=sum_send.at[way, k, p], recv_sem=sum_recv.at[way, k, p],
            device_id={"group": next_g[way]}, device_id_type=MESH)

    def pass_on(k):
        return pltpu.make_async_remote_copy(
            src_ref=txt_all.at[at(k)], dst_ref=txt_all.at[at(k)],
            send_sem=pass_send.at[k], recv_sem=d_recv.at[BLOCK, k],
            device_id={"dp": side}, device_id_type=MESH)

    def side_copy(c):
        return pltpu.make_async_remote_copy(
            src_ref=gt_send.at[c * per + (per - 1 - core)], dst_ref=gt_side.at[c],
            send_sem=side_send.at[c], recv_sem=side_recv.at[c],
            device_id={"dp": side}, device_id_type=MESH)

    def g_peer(o):
        return lax.rem(g + o, gn)

    def d_peer(o):
        return lax.rem(d + o, dn)

    def at(k, n=rows):
        return pl.ds(pl.multiple_of(k * n, n), n)

    def g_copy(kind, src, dst, to, slot):
        return pltpu.make_async_remote_copy(
            src_ref=src, dst_ref=dst, send_sem=g_send.at[kind, to], recv_sem=g_recv.at[kind, slot],
            device_id={"group": to}, device_id_type=MESH)

    def d_copy(kind, src, dst, to, slot):
        return pltpu.make_async_remote_copy(
            src_ref=src, dst_ref=dst, send_sem=d_send.at[kind, to], recv_sem=d_recv.at[kind, slot],
            device_id={"dp": to}, device_id_type=MESH)

    barrier = pltpu.get_barrier_semaphore()
    each(gn - 1, lambda i: pl.semaphore_signal(
        barrier, inc=1, device_id={"group": g_peer(i + 1)}, device_id_type=MESH))
    each(dn - 1, lambda i: pl.semaphore_signal(
        barrier, inc=1, device_id={"dp": d_peer(i + 1)}, device_id_type=MESH))
    pl.semaphore_wait(barrier, gn + dn - 2)

    def text_block(k):
        return d_copy(BLOCK, texts, txt_all.at[at(d)], k, d)

    @pl.when(g < gn - 1)
    def _():
        first_hop(UP).start()

    @pl.when(g > 0)
    def _():
        first_hop(DOWN).start()

    each(chunks - 1, lambda i: text_block(c_peer(i + 1) * per + core).start())
    if per == 2:
        text_block(side).start()
    img_all[at(g), :] = images[...]
    txt_all[at(d), :] = texts[...]
    s = jnp.exp(log_scale[...])
    eye = (lax.broadcasted_iota(jnp.int32, (rows, rows), 0)
           == lax.broadcasted_iota(jnp.int32, (rows, rows), 1))

    def relay_images(j):
        @pl.when(g - j >= 0)
        def _():
            hop(UP, g - j).wait_recv()

            @pl.when(g < gn - 1)
            def _():
                hop(UP, g - j).start()

        @pl.when(g + j < gn)
        def _():
            hop(DOWN, g + j).wait_recv()

            @pl.when(g > 0)
            def _():
                hop(DOWN, g + j).start()

    def relay_text(i):
        k = c_peer(i + 1) * per + core
        d_copy(BLOCK, texts, txt_all.at[at(k)], k, k).wait_recv()
        if per == 2:
            pass_on(k).start()

    for j in range(1, gn):
        relay_images(j)
        if j == 1:
            each(chunks - 1, relay_text)
    if gn == 1:
        each(chunks - 1, relay_text)

    def logits_chunk(i):
        c = c_peer(i)
        if per == 2:
            k = c * per + (per - 1 - core)
            d_copy(BLOCK, texts, txt_all.at[at(k)], k, k).wait_recv()
        part = s * lax.dot_general(img_all[...], txt_all[at(c, wide), :], NT, preferred_element_type=F32)
        logits[:, at(c, wide)] = part
        high = jnp.max(part, axis=0, keepdims=True)
        col_stat[d, 0:1, at(c, wide)] = high
        col_stat[d, 1:2, at(c, wide)] = jnp.sum(jnp.exp(part - high), axis=0, keepdims=True)
        if isinstance(i, int) and i == 0:
            top[...] = part
        else:
            top[...] = jnp.maximum(top[...], part)

    if chunks > 8:
        top[...] = jnp.full(top.shape, -jnp.inf, F32)
    each(chunks, logits_chunk)
    each(dn - 1, lambda i: d_copy(STAT, col_stat.at[d], col_stat.at[d], d_peer(i + 1), d).start())

    def flat(col):
        return jnp.sum(jnp.where(eye, col, 0.0), axis=0, keepdims=True)

    def stand(line):
        return jnp.sum(jnp.where(eye, line, 0.0), axis=1, keepdims=True)

    for k in range(gn):
        band = pl.ds(k * rows, rows)
        high = jnp.max(top[band, :], axis=1, keepdims=True)
        acc[...] = jnp.zeros(acc.shape, F32)

        def add(c):
            acc[...] += jnp.exp(logits[band, at(c, wide)] - high)

        each(chunks, add)
        row_stat[g, 0:1, band] = flat(high)
        row_stat[g, 1:2, band] = flat(jnp.sum(acc[...], axis=1, keepdims=True))
    each(gn - 1, lambda i: g_copy(STAT, row_stat.at[g], row_stat.at[g], g_peer(i + 1), g).start())

    def wait_row(i):
        k = g_peer(i + 1)
        g_copy(STAT, row_stat.at[k], row_stat.at[k], k, k).wait_recv()

    def wait_col(i):
        k = d_peer(i + 1)
        d_copy(STAT, col_stat.at[k], col_stat.at[k], k, k).wait_recv()

    def lse(stat):
        high = jnp.max(stat[:, 0, :], axis=0, keepdims=True)
        return high + jnp.log(jnp.sum(stat[:, 1, :] * jnp.exp(stat[:, 0, :] - high), axis=0, keepdims=True))

    each(dn - 1, wait_col)
    col_lse[...] = lse(col_stat)
    each(gn - 1, wait_row)
    row_lse[...] = lse(row_stat)

    acc[...] = jnp.zeros(acc.shape, F32)
    across = 4 * dn * rows
    step_of = (lax.broadcasted_iota(jnp.int32, (rows, wide), 1)
               - lax.broadcasted_iota(jnp.int32, (rows, wide), 0))
    order = sorted(range(gn), key=lambda t: (-abs(2 * t - gn + 1), -t))
    for k in order:
        line = stand(row_lse[0:1, at(k)])

        def weigh(c):
            part = logits[at(k), at(c, wide)]
            w = 0.5 * (jnp.exp(part - line) + jnp.exp(part - col_lse[0:1, at(c, wide)]))
            w = w - jnp.where(step_of == jnp.where(k == g, d * rows - c * wide, -across), 1.0, 0.0)
            acc[...] += w * part
            weights[at(k), at(c, wide)] = w.astype(jnp.bfloat16)

        each(chunks, weigh)
        gi_send[k] = lax.dot_general(weights[at(k), :], txt_all[...], NN, preferred_element_type=F32)
        for p in range(PIECES):
            if k > 0:
                @pl.when(g == 0)
                def _():
                    sum_hop(UP, k, p).start()
            if k < gn - 1:
                @pl.when(g == gn - 1)
                def _():
                    sum_hop(DOWN, k, p).start()

    own = logits[at(g), at(d)]
    pairs = jnp.sum(jnp.where(eye, own, 0.0), axis=0, keepdims=True)
    loss_part = jnp.sum(row_lse[0:1, at(g)] + col_lse[0:1, at(d)] - 2.0 * pairs, axis=1, keepdims=True)
    scale_part = jnp.sum(jnp.sum(acc[...], axis=0, keepdims=True), axis=1, keepdims=True)
    first = lax.broadcasted_iota(jnp.int32, (8, 128), 1) == 0
    sc_group[g] = jnp.where(first, loss_part, scale_part)
    each(gn - 1, lambda i: g_copy(SCALAR, sc_group.at[g], sc_group.at[g], g_peer(i + 1), g).start())

    def share(i):
        c = c_peer(1 + i)
        k = c * per + core
        if per == 2:
            side_copy(c).wait_recv()
            gt_send[k] += gt_side[c]

        @pl.when(c != chip)
        def _():
            pltpu.make_async_remote_copy(
                src_ref=gt_send.at[k], dst_ref=gt_recv.at[chip],
                send_sem=d_send.at[GRAD, c], recv_sem=d_recv.at[GRAD, chip],
                device_id={"dp": k}, device_id_type=MESH).start()

    def text_chunk(i):
        c = c_peer(1 + i)
        part = lax.dot_general(weights[:, at(c, wide)], img_all[...], TN, preferred_element_type=F32)
        for j in range(per):
            gt_send[c * per + j] = part[j * rows:(j + 1) * rows]
        if per == 2:
            side_copy(c).start()
        if isinstance(i, int):
            if i > 0:
                share(i - 1)
        else:
            @pl.when(i > 0)
            def _():
                share(i - 1)

    each(chunks, text_chunk)
    share(chunks - 1)

    def add_sum(way, k, p):
        piece = pl.ds(p * (rows // PIECES), rows // PIECES)
        sum_hop(way, k, p).wait_recv()
        gi_send[k, piece] += gi_recv[way, k, piece]

    for j in range(gn - 1):
        for p in range(PIECES):
            @pl.when((g > 0) & (gn - 1 - j > g))
            def _():
                add_sum(UP, gn - 1 - j, p)
                sum_hop(UP, gn - 1 - j, p).start()

            @pl.when((g < gn - 1) & (j < g))
            def _():
                add_sum(DOWN, j, p)
                sum_hop(DOWN, j, p).start()

    def wait_sc_group(i):
        k = g_peer(i + 1)
        g_copy(SCALAR, sc_group.at[k], sc_group.at[k], k, k).wait_recv()

    each(gn - 1, wait_sc_group)
    sc_dp[d] = jnp.sum(sc_group[...], axis=0)
    each(dn - 1, lambda i: d_copy(SCALAR, sc_dp.at[d], sc_dp.at[d], d_peer(i + 1), d).start())

    def take_d(i):
        c = c_peer(i + 1)
        pltpu.make_async_remote_copy(
            src_ref=gt_recv.at[c], dst_ref=gt_recv.at[c],
            send_sem=d_send.at[GRAD, c], recv_sem=d_recv.at[GRAD, c],
            device_id={"dp": c * per + core}, device_id_type=MESH).wait_recv()
        gt_send[d] += gt_recv[c]

    each(chunks - 1, take_d)
    gt_out[...] = (s * gt_send[d]).astype(gt_out.dtype)

    for p in range(PIECES):
        @pl.when(g > 0)
        def _():
            add_sum(UP, g, p)

        @pl.when(g < gn - 1)
        def _():
            add_sum(DOWN, g, p)

    gi_out[...] = (s * gi_send[g]).astype(gi_out.dtype)

    def wait_sc_dp(i):
        k = d_peer(i + 1)
        d_copy(SCALAR, sc_dp.at[k], sc_dp.at[k], k, k).wait_recv()

    each(dn - 1, wait_sc_dp)
    total = jnp.sum(sc_dp[...], axis=0)
    pair_total = gn * dn * rows
    loss_out[...] = total[0:1, 0:1] / (2.0 * pair_total)
    scale_out[...] = total[0:1, 1:2] / pair_total

    def end_g(i):
        k = g_peer(i + 1)
        g_copy(STAT, row_stat.at[g], row_stat.at[g], k, g).wait_send()
        g_copy(SCALAR, sc_group.at[g], sc_group.at[g], k, g).wait_send()

    def end_d(i):
        k = d_peer(i + 1)
        d_copy(STAT, col_stat.at[d], col_stat.at[d], k, d).wait_send()
        d_copy(SCALAR, sc_dp.at[d], sc_dp.at[d], k, d).wait_send()

    def end_c(i):
        c = c_peer(i + 1)
        k = c * per + core
        text_block(k).wait_send()
        if per == 2:
            pass_on(k).wait_send()
            side_copy(c).wait_send()
        pltpu.make_async_remote_copy(
            src_ref=gt_send.at[k], dst_ref=gt_recv.at[chip],
            send_sem=d_send.at[GRAD, c], recv_sem=d_recv.at[GRAD, chip],
            device_id={"dp": k}, device_id_type=MESH).wait_send()

    each(gn - 1, end_g)
    each(dn - 1, end_d)
    each(chunks - 1, end_c)
    if per == 2:
        text_block(side).wait_send()
        side_copy(chip).wait_send()

    for k in range(gn):
        @pl.when((g < gn - 1) & (k <= g))
        def _():
            hop(UP, k).wait_send()

        @pl.when((g > 0) & (k >= g))
        def _():
            hop(DOWN, k).wait_send()

        for p in range(PIECES):
            @pl.when(k > g)
            def _():
                sum_hop(UP, k, p).wait_send()

            @pl.when(k < g)
            def _():
                sum_hop(DOWN, k, p).wait_send()


def body(gn, dn, images, texts, log_scale):
    rows, width = images.shape
    high, across = gn * rows, dn * rows
    wide = 2 * rows if dn % 2 == 0 else rows
    chunks = across // wide
    vmem = pl.BlockSpec(memory_space=pltpu.VMEM)
    gi, gt, loss, scale = pl.pallas_call(
        functools.partial(kernel, gn, dn),
        out_shape=(
            jax.ShapeDtypeStruct(images.shape, images.dtype),
            jax.ShapeDtypeStruct(texts.shape, texts.dtype),
            jax.ShapeDtypeStruct((1, 1), F32),
            jax.ShapeDtypeStruct((1, 1), F32),
        ),
        in_specs=[vmem] * 3,
        out_specs=(vmem,) * 4,
        scratch_shapes=[
            pltpu.VMEM((high, width), images.dtype),
            pltpu.VMEM((across, width), texts.dtype),
            pltpu.VMEM((high, across), F32),
            pltpu.VMEM((high, across), jnp.bfloat16),
            pltpu.VMEM((gn, 2, high), F32),
            pltpu.VMEM((dn, 2, across), F32),
            pltpu.VMEM((high, wide), F32),
            pltpu.VMEM((rows, wide), F32),
            pltpu.VMEM((1, high), F32),
            pltpu.VMEM((1, across), F32),
            pltpu.VMEM((gn, rows, width), F32),
            pltpu.VMEM((2, gn, rows, width), F32),
            pltpu.VMEM((dn, rows, width), F32),
            pltpu.VMEM((chunks, rows, width), F32),
            pltpu.VMEM((chunks, rows, width), F32),
            pltpu.VMEM((gn, 8, 128), F32),
            pltpu.VMEM((dn, 8, 128), F32),
            pltpu.SemaphoreType.DMA((4, gn)),
            pltpu.SemaphoreType.DMA((4, gn)),
            pltpu.SemaphoreType.DMA((4, dn)),
            pltpu.SemaphoreType.DMA((4, dn)),
            pltpu.SemaphoreType.DMA((2, gn)),
            pltpu.SemaphoreType.DMA((2, gn, PIECES)),
            pltpu.SemaphoreType.DMA((2, gn, PIECES)),
            pltpu.SemaphoreType.DMA((chunks,)),
            pltpu.SemaphoreType.DMA((dn,)),
            pltpu.SemaphoreType.DMA((chunks,)),
        ],
        compiler_params=pltpu.CompilerParams(
            collective_id=0, has_side_effects=True, vmem_limit_bytes=60 * 1024 * 1024),
    )(images, texts, log_scale.reshape(1, 1))
    return gi, gt, loss.reshape(()), scale.reshape(())


def solution(mesh):
    gn, dn = mesh.shape["group"], mesh.shape["dp"]
    spec = P(("dp", "group"), None)
    return jax.shard_map(
        functools.partial(body, gn, dn), mesh=mesh, in_specs=(spec, spec, P()),
        out_specs=(spec, spec, P(), P()), check_vma=False)
```

```python
import functools

import jax
import jax.numpy as jnp
from jax import lax
from jax.experimental import pallas as pl
from jax.experimental.pallas import tpu as pltpu
from jax.sharding import PartitionSpec as P

MESH = pl.DeviceIdType.MESH
NT = (((1,), (1,)), ((), ()))
NN = (((1,), (0,)), ((), ()))
TN = (((0,), (0,)), ((), ()))
F32 = jnp.float32
BLOCK, STAT, GRAD, SCALAR = range(4)
UP, DOWN = range(2)
PIECES = 1


def each(count, step):
    if count <= 8:
        for i in range(count):
            step(i)
    else:
        lax.fori_loop(0, count, lambda i, c: (step(i), c)[1], 0)


def kernel(
    gn, dn, images, texts, log_scale, gi_out, gt_out, loss_out, scale_out,
    img_all, txt_all, logits, weights, row_stat, col_stat, top, acc, row_lse, col_lse,
    gi_send, gi_recv, gt_send, gt_recv, gt_side, sc_group, sc_dp, g_send, g_recv, d_send, d_recv,
    hop_send, sum_send, sum_recv, side_send, pass_send, side_recv,
):
    rows, width = images.shape
    g = lax.axis_index("group")
    d = lax.axis_index("dp")
    wide = 2 * rows if dn % 2 == 0 else rows
    per = wide // rows
    chunks = dn // per

    chip, core = d // per, lax.rem(d, per)
    side = chip * per + (per - 1 - core)
    next_g = (lax.min(g + 1, gn - 1), lax.max(g - 1, 0))

    def c_peer(o):
        return lax.rem(chip + o, chunks)

    def hop(way, k):
        return pltpu.make_async_remote_copy(
            src_ref=img_all.at[at(k)], dst_ref=img_all.at[at(k)],
            send_sem=hop_send.at[way, k], recv_sem=g_recv.at[BLOCK, k],
            device_id={"group": next_g[way]}, device_id_type=MESH)

    def first_hop(way):
        return pltpu.make_async_remote_copy(
            src_ref=images, dst_ref=img_all.at[at(g)],
            send_sem=hop_send.at[way, g], recv_sem=g_recv.at[BLOCK, g],
            device_id={"group": next_g[way]}, device_id_type=MESH)

    def sum_hop(way, k, p):
        piece = pl.ds(p * (rows // PIECES), rows // PIECES)
        return pltpu.make_async_remote_copy(
            src_ref=gi_send.at[k, piece], dst_ref=gi_recv.at[way, k, piece],
            send_sem=sum_send.at[way, k, p], recv_sem=sum_recv.at[way, k, p],
            device_id={"group": next_g[way]}, device_id_type=MESH)

    def pass_on(k):
        return pltpu.make_async_remote_copy(
            src_ref=txt_all.at[at(k)], dst_ref=txt_all.at[at(k)],
            send_sem=pass_send.at[k], recv_sem=d_recv.at[BLOCK, k],
            device_id={"dp": side}, device_id_type=MESH)

    def side_copy(c):
        return pltpu.make_async_remote_copy(
            src_ref=gt_send.at[c * per + (per - 1 - core)], dst_ref=gt_side.at[c],
            send_sem=side_send.at[c], recv_sem=side_recv.at[c],
            device_id={"dp": side}, device_id_type=MESH)

    def g_peer(o):
        return lax.rem(g + o, gn)

    def d_peer(o):
        return lax.rem(d + o, dn)

    def at(k, n=rows):
        return pl.ds(pl.multiple_of(k * n, n), n)

    def g_copy(kind, src, dst, to, slot):
        return pltpu.make_async_remote_copy(
            src_ref=src, dst_ref=dst, send_sem=g_send.at[kind, to], recv_sem=g_recv.at[kind, slot],
            device_id={"group": to}, device_id_type=MESH)

    def d_copy(kind, src, dst, to, slot):
        return pltpu.make_async_remote_copy(
            src_ref=src, dst_ref=dst, send_sem=d_send.at[kind, to], recv_sem=d_recv.at[kind, slot],
            device_id={"dp": to}, device_id_type=MESH)

    barrier = pltpu.get_barrier_semaphore()
    each(gn - 1, lambda i: pl.semaphore_signal(
        barrier, inc=1, device_id={"group": g_peer(i + 1)}, device_id_type=MESH))
    each(dn - 1, lambda i: pl.semaphore_signal(
        barrier, inc=1, device_id={"dp": d_peer(i + 1)}, device_id_type=MESH))
    pl.semaphore_wait(barrier, gn + dn - 2)

    def text_block(k):
        return d_copy(BLOCK, texts, txt_all.at[at(d)], k, d)

    @pl.when(g < gn - 1)
    def _():
        first_hop(UP).start()

    @pl.when(g > 0)
    def _():
        first_hop(DOWN).start()

    each(chunks - 1, lambda i: text_block(c_peer(i + 1) * per + core).start())
    if per == 2:
        text_block(side).start()
    img_all[at(g), :] = images[...]
    txt_all[at(d), :] = texts[...]
    s = jnp.exp(log_scale[...])
    eye = (lax.broadcasted_iota(jnp.int32, (rows, rows), 0)
           == lax.broadcasted_iota(jnp.int32, (rows, rows), 1))

    def relay_images(j):
        @pl.when(g - j >= 0)
        def _():
            hop(UP, g - j).wait_recv()

            @pl.when(g < gn - 1)
            def _():
                hop(UP, g - j).start()

        @pl.when(g + j < gn)
        def _():
            hop(DOWN, g + j).wait_recv()

            @pl.when(g > 0)
            def _():
                hop(DOWN, g + j).start()

    def relay_text(i):
        k = c_peer(i + 1) * per + core
        d_copy(BLOCK, texts, txt_all.at[at(k)], k, k).wait_recv()
        if per == 2:
            pass_on(k).start()

    def flat(col):
        return jnp.sum(jnp.where(eye, col, 0.0), axis=0, keepdims=True)

    def stand(line):
        return jnp.sum(jnp.where(eye, line, 0.0), axis=1, keepdims=True)

    def wait_side(i):
        k = c_peer(i) * per + (per - 1 - core)
        d_copy(BLOCK, texts, txt_all.at[at(k)], k, k).wait_recv()

    def band_logits(k, first=False):
        top[...] = jnp.full(top.shape, -jnp.inf, F32)
        acc[...] = jnp.zeros(acc.shape, F32)

        def fill(c):
            cols = at(c, wide)
            part = s * lax.dot_general(img_all[at(k), :], txt_all[cols, :], NT, preferred_element_type=F32)
            logits[at(k), cols] = part
            top[...] = jnp.maximum(top[...], part)
            peak = jnp.max(part, axis=0, keepdims=True)
            if first:
                col_stat[d, 0:1, cols] = peak
                col_stat[d, 1:2, cols] = jnp.sum(jnp.exp(part - peak), axis=0, keepdims=True)
            else:
                old = col_stat[d, 0:1, cols]
                peak = jnp.maximum(old, peak)
                col_stat[d, 0:1, cols] = peak
                col_stat[d, 1:2, cols] = (col_stat[d, 1:2, cols] * jnp.exp(old - peak)
                                          + jnp.sum(jnp.exp(part - peak), axis=0, keepdims=True))

        each(chunks, fill)
        high = jnp.max(top[...], axis=1, keepdims=True)

        def add(c):
            acc[...] += jnp.exp(logits[at(k), at(c, wide)] - high)

        each(chunks, add)
        row_stat[g, 0:1, at(k)] = flat(high)
        row_stat[g, 1:2, at(k)] = flat(jnp.sum(acc[...], axis=1, keepdims=True))

    def both_bands(j):
        @pl.when(g - j >= 0)
        def _():
            band_logits(g - j)

        @pl.when(g + j < gn)
        def _():
            band_logits(g + j)

    for j in range(1, gn - 1):
        relay_images(j)
        if j == 1:
            each(chunks - 1, relay_text)
    if gn <= 2:
        each(chunks - 1, relay_text)
    if per == 2:
        each(chunks, wait_side)
    band_logits(g, True)
    for j in range(1, gn - 1):
        both_bands(j)
    if gn > 1:
        relay_images(gn - 1)
        both_bands(gn - 1)
    each(dn - 1, lambda i: d_copy(STAT, col_stat.at[d], col_stat.at[d], d_peer(i + 1), d).start())
    each(gn - 1, lambda i: g_copy(STAT, row_stat.at[g], row_stat.at[g], g_peer(i + 1), g).start())

    def wait_row(i):
        k = g_peer(i + 1)
        g_copy(STAT, row_stat.at[k], row_stat.at[k], k, k).wait_recv()

    def wait_col(i):
        k = d_peer(i + 1)
        d_copy(STAT, col_stat.at[k], col_stat.at[k], k, k).wait_recv()

    def lse(stat):
        high = jnp.max(stat[:, 0, :], axis=0, keepdims=True)
        return high + jnp.log(jnp.sum(stat[:, 1, :] * jnp.exp(stat[:, 0, :] - high), axis=0, keepdims=True))

    each(dn - 1, wait_col)
    col_lse[...] = lse(col_stat)
    each(gn - 1, wait_row)
    row_lse[...] = lse(row_stat)

    acc[...] = jnp.zeros(acc.shape, F32)
    across = 4 * dn * rows
    step_of = (lax.broadcasted_iota(jnp.int32, (rows, wide), 1)
               - lax.broadcasted_iota(jnp.int32, (rows, wide), 0))
    order = sorted(range(gn), key=lambda t: (-abs(2 * t - gn + 1), -t))


    def weigh_band(k):
        line = stand(row_lse[0:1, at(k)])

        def weigh(c):
            part = logits[at(k), at(c, wide)]
            w = 0.5 * (jnp.exp(part - line) + jnp.exp(part - col_lse[0:1, at(c, wide)]))
            w = w - jnp.where(step_of == jnp.where(k == g, d * rows - c * wide, -across), 1.0, 0.0)
            acc[...] += w * part
            weights[at(k), at(c, wide)] = w.astype(jnp.bfloat16)

        each(chunks, weigh)

    def give(k):
        gi_send[k] = lax.dot_general(weights[at(k), :], txt_all[...], NN, preferred_element_type=F32)
        for p in range(PIECES):
            if k > 0:
                @pl.when(g == 0)
                def _():
                    sum_hop(UP, k, p).start()
            if k < gn - 1:
                @pl.when(g == gn - 1)
                def _():
                    sum_hop(DOWN, k, p).start()

    for k in order[:2]:
        weigh_band(k)
        give(k)
    for k in order[2:]:
        weigh_band(k)

    own = logits[at(g), at(d)]
    pairs = jnp.sum(jnp.where(eye, own, 0.0), axis=0, keepdims=True)
    loss_part = jnp.sum(row_lse[0:1, at(g)] + col_lse[0:1, at(d)] - 2.0 * pairs, axis=1, keepdims=True)
    scale_part = jnp.sum(jnp.sum(acc[...], axis=0, keepdims=True), axis=1, keepdims=True)
    first = lax.broadcasted_iota(jnp.int32, (8, 128), 1) == 0
    sc_group[g] = jnp.where(first, loss_part, scale_part)
    each(gn - 1, lambda i: g_copy(SCALAR, sc_group.at[g], sc_group.at[g], g_peer(i + 1), g).start())

    for k in order[2:]:
        give(k)

    def share(i):
        c = c_peer(1 + i)
        k = c * per + core
        if per == 2:
            side_copy(c).wait_recv()
            gt_send[k] += gt_side[c]

        @pl.when(c != chip)
        def _():
            pltpu.make_async_remote_copy(
                src_ref=gt_send.at[k], dst_ref=gt_recv.at[chip],
                send_sem=d_send.at[GRAD, c], recv_sem=d_recv.at[GRAD, chip],
                device_id={"dp": k}, device_id_type=MESH).start()

    def text_chunk(i):
        c = c_peer(1 + i)
        part = lax.dot_general(weights[:, at(c, wide)], img_all[...], TN, preferred_element_type=F32)
        for j in range(per):
            gt_send[c * per + j] = part[j * rows:(j + 1) * rows]
        if per == 2:
            side_copy(c).start()
        if isinstance(i, int):
            if i > 0:
                share(i - 1)
        else:
            @pl.when(i > 0)
            def _():
                share(i - 1)

    each(chunks, text_chunk)
    share(chunks - 1)

    def add_sum(way, k, p):
        piece = pl.ds(p * (rows // PIECES), rows // PIECES)
        sum_hop(way, k, p).wait_recv()
        gi_send[k, piece] += gi_recv[way, k, piece]

    def wait_sc_group(i):
        k = g_peer(i + 1)
        g_copy(SCALAR, sc_group.at[k], sc_group.at[k], k, k).wait_recv()

    def pass_scalars():
        each(gn - 1, wait_sc_group)
        sc_dp[d] = jnp.sum(sc_group[...], axis=0)
        each(dn - 1, lambda i: d_copy(SCALAR, sc_dp.at[d], sc_dp.at[d], d_peer(i + 1), d).start())

    if gn == 1:
        pass_scalars()
    for j in range(gn - 1):
        for p in range(PIECES):
            @pl.when((g > 0) & (gn - 1 - j > g))
            def _():
                add_sum(UP, gn - 1 - j, p)
                sum_hop(UP, gn - 1 - j, p).start()

            @pl.when((g < gn - 1) & (j < g))
            def _():
                add_sum(DOWN, j, p)
                sum_hop(DOWN, j, p).start()

        if j == 0:
            pass_scalars()

    def take_d(i):
        c = c_peer(i + 1)
        pltpu.make_async_remote_copy(
            src_ref=gt_recv.at[c], dst_ref=gt_recv.at[c],
            send_sem=d_send.at[GRAD, c], recv_sem=d_recv.at[GRAD, c],
            device_id={"dp": c * per + core}, device_id_type=MESH).wait_recv()
        gt_send[d] += gt_recv[c]

    each(chunks - 1, take_d)
    gt_out[...] = (s * gt_send[d]).astype(gt_out.dtype)

    for p in range(PIECES):
        @pl.when(g > 0)
        def _():
            add_sum(UP, g, p)

        @pl.when(g < gn - 1)
        def _():
            add_sum(DOWN, g, p)

    gi_out[...] = (s * gi_send[g]).astype(gi_out.dtype)

    def wait_sc_dp(i):
        k = d_peer(i + 1)
        d_copy(SCALAR, sc_dp.at[k], sc_dp.at[k], k, k).wait_recv()

    each(dn - 1, wait_sc_dp)
    total = jnp.sum(sc_dp[...], axis=0)
    pair_total = gn * dn * rows
    loss_out[...] = total[0:1, 0:1] / (2.0 * pair_total)
    scale_out[...] = total[0:1, 1:2] / pair_total

    def end_g(i):
        k = g_peer(i + 1)
        g_copy(STAT, row_stat.at[g], row_stat.at[g], k, g).wait_send()
        g_copy(SCALAR, sc_group.at[g], sc_group.at[g], k, g).wait_send()

    def end_d(i):
        k = d_peer(i + 1)
        d_copy(STAT, col_stat.at[d], col_stat.at[d], k, d).wait_send()
        d_copy(SCALAR, sc_dp.at[d], sc_dp.at[d], k, d).wait_send()

    def end_c(i):
        c = c_peer(i + 1)
        k = c * per + core
        text_block(k).wait_send()
        if per == 2:
            pass_on(k).wait_send()
            side_copy(c).wait_send()
        pltpu.make_async_remote_copy(
            src_ref=gt_send.at[k], dst_ref=gt_recv.at[chip],
            send_sem=d_send.at[GRAD, c], recv_sem=d_recv.at[GRAD, chip],
            device_id={"dp": k}, device_id_type=MESH).wait_send()

    each(gn - 1, end_g)
    each(dn - 1, end_d)
    each(chunks - 1, end_c)
    if per == 2:
        text_block(side).wait_send()
        side_copy(chip).wait_send()

    for k in range(gn):
        @pl.when((g < gn - 1) & (k <= g))
        def _():
            hop(UP, k).wait_send()

        @pl.when((g > 0) & (k >= g))
        def _():
            hop(DOWN, k).wait_send()

        for p in range(PIECES):
            @pl.when(k > g)
            def _():
                sum_hop(UP, k, p).wait_send()

            @pl.when(k < g)
            def _():
                sum_hop(DOWN, k, p).wait_send()


def body(gn, dn, images, texts, log_scale):
    rows, width = images.shape
    high, across = gn * rows, dn * rows
    wide = 2 * rows if dn % 2 == 0 else rows
    chunks = across // wide
    vmem = pl.BlockSpec(memory_space=pltpu.VMEM)
    gi, gt, loss, scale = pl.pallas_call(
        functools.partial(kernel, gn, dn),
        out_shape=(
            jax.ShapeDtypeStruct(images.shape, images.dtype),
            jax.ShapeDtypeStruct(texts.shape, texts.dtype),
            jax.ShapeDtypeStruct((1, 1), F32),
            jax.ShapeDtypeStruct((1, 1), F32),
        ),
        in_specs=[vmem] * 3,
        out_specs=(vmem,) * 4,
        scratch_shapes=[
            pltpu.VMEM((high, width), images.dtype),
            pltpu.VMEM((across, width), texts.dtype),
            pltpu.VMEM((high, across), F32),
            pltpu.VMEM((high, across), jnp.bfloat16),
            pltpu.VMEM((gn, 2, high), F32),
            pltpu.VMEM((dn, 2, across), F32),
            pltpu.VMEM((rows, wide), F32),
            pltpu.VMEM((rows, wide), F32),
            pltpu.VMEM((1, high), F32),
            pltpu.VMEM((1, across), F32),
            pltpu.VMEM((gn, rows, width), F32),
            pltpu.VMEM((2, gn, rows, width), F32),
            pltpu.VMEM((dn, rows, width), F32),
            pltpu.VMEM((chunks, rows, width), F32),
            pltpu.VMEM((chunks, rows, width), F32),
            pltpu.VMEM((gn, 8, 128), F32),
            pltpu.VMEM((dn, 8, 128), F32),
            pltpu.SemaphoreType.DMA((4, gn)),
            pltpu.SemaphoreType.DMA((4, gn)),
            pltpu.SemaphoreType.DMA((4, dn)),
            pltpu.SemaphoreType.DMA((4, dn)),
            pltpu.SemaphoreType.DMA((2, gn)),
            pltpu.SemaphoreType.DMA((2, gn, PIECES)),
            pltpu.SemaphoreType.DMA((2, gn, PIECES)),
            pltpu.SemaphoreType.DMA((chunks,)),
            pltpu.SemaphoreType.DMA((dn,)),
            pltpu.SemaphoreType.DMA((chunks,)),
        ],
        compiler_params=pltpu.CompilerParams(
            collective_id=0, has_side_effects=True, vmem_limit_bytes=60 * 1024 * 1024),
    )(images, texts, log_scale.reshape(1, 1))
    return gi, gt, loss.reshape(()), scale.reshape(())


def solution(mesh):
    gn, dn = mesh.shape["group"], mesh.shape["dp"]
    spec = P(("dp", "group"), None)
    return jax.shard_map(
        functools.partial(body, gn, dn), mesh=mesh, in_specs=(spec, spec, P()),
        out_specs=(spec, spec, P(), P()), check_vma=False)
```
